32 devices in a mesh: gx: 8 (over z, y), gy: 4 (over x, core).
Axes of the slice: x: 2, y: 2, z: 4, core: 2. Of those that a mesh axis runs over, the one named last changes fastest.
Arguments:
- loads: float32 [64, 49152], P(None, ('gx', 'gy')), may hold values from -6 to 6
- guess: float32 [64, 49152], P(None, ('gx', 'gy')), may hold values from -4 to 4
- mass: float32 [49152], P(('gx', 'gy')), may hold values from 0.5 to 4
- moduli: float32 [49152], P(('gx', 'gy')), may hold values from 0.3 to 3
- tiles: float32 [1280, 256, 256], P(('gx', 'gy')), may hold values from -0.21875 to 0.21875
- tile_row: int32 [1280], P(('gx', 'gy')), may hold values from -1 to 5, as said below
- tile_col: int32 [1280], P(('gx', 'gy')), may hold values from 0 to 21, as said below
- send_list: int32 [32, 4, 4], P(('gx', 'gy')), may hold values from -1 to 5, as said below
Outputs:
- solution: float32 [64, 49152], P(None, ('gx', 'gy'))
- residual: float32 [64, 49152], P(None, ('gx', 'gy'))
The draws below stay inside these ranges and needn't reach their ends.
Inputs may be any that keep to these rules, and one draw needn't show every extreme that they name: `tile_row`: strain block (of the tile's own device) of each slot, -1 for an unused slot. A device's used slots come first; slot r below 6 holds the diagonal tile of block r; some device uses all 40 slots. `tile_col`: column block of each slot in its device's extended numbering: below 6 an own block; 6 + g * 4 + k the k-th entry of the list that neighbour g (0 below along gx, 1 above along gx, 2 below along gy, 3 above along gy) sends to this device. Used slots read only entries that are not -1, every such entry is read by some slot, unused slots hold 0. `send_list`: for each device and each neighbour in the order below gx, above gx, below gy, above gy: distinct own blocks to send, padded with -1 at the end; all -1 toward a missing neighbour; some lists are full.
All inputs are finite; a program needn't handle non-finite values.
Results may differ from the reference program's by a relative error of at most 0.0003.
Values sent between devices are 32-bit elements; how exact they have to be, the bound alone decides.
A program may use at most 128 MiB of HBM per device.

```python
import math
import jax
import jax.numpy as jnp
from jax import lax

TB = 256
RB = 6
HALO = 4
TILE_SLOTS = 40
NRHS = 64
ITERS = 2
DOFS = 49152
TILES = 1280
N_GX = 8
N_GY = 4


def layout(key):
    devices_all = N_GX * N_GY
    flat = jnp.arange(devices_all, dtype=jnp.int32)
    along_x = flat // N_GY
    along_y = flat % N_GY
    counts = jax.random.randint(jax.random.fold_in(key, 101), (devices_all, 4), 1, HALO + 1)
    counts = jnp.where((flat % 5 == 0)[:, None], HALO, counts)
    present = jnp.stack([along_x > 0, along_x < N_GX - 1, along_y > 0, along_y < N_GY - 1], axis=1)
    counts = jnp.where(present, counts, 0).astype(jnp.int32)
    scores = jax.random.randint(jax.random.fold_in(key, 102), (devices_all, 4, RB), 0, 1 << 20) * RB + jnp.arange(RB, dtype=jnp.int32)
    order = jnp.argsort(scores, axis=-1)[:, :, :HALO].astype(jnp.int32)
    send_list = jnp.where(jnp.arange(HALO, dtype=jnp.int32) < counts[:, :, None], order, -1)
    grid = counts.reshape(N_GX, N_GY, 4)
    zero_row = jnp.zeros((1, N_GY), jnp.int32)
    zero_col = jnp.zeros((N_GX, 1), jnp.int32)
    from_lower_x = jnp.concatenate([zero_row, grid[:-1, :, 1]], 0)
    from_upper_x = jnp.concatenate([grid[1:, :, 0], zero_row], 0)
    from_lower_y = jnp.concatenate([zero_col, grid[:, :-1, 3]], 1)
    from_upper_y = jnp.concatenate([grid[:, 1:, 2], zero_col], 1)
    incoming = jnp.stack([from_lower_x, from_upper_x, from_lower_y, from_upper_y], -1).reshape(devices_all, 4)
    halo_index = jnp.arange(4 * HALO, dtype=jnp.int32)
    halo_live = (halo_index % HALO)[None, :] < incoming[:, halo_index // HALO]
    column_live = jnp.concatenate([jnp.ones((devices_all, RB), bool), halo_live], 1)
    needed = RB + jnp.sum(incoming, axis=1)
    spare = TILE_SLOTS - needed + 1
    extra_one = jax.random.randint(jax.random.fold_in(key, 103), (devices_all,), 0, spare)
    extra_two = jax.random.randint(jax.random.fold_in(key, 104), (devices_all,), 0, spare)
    extra_three = jax.random.randint(jax.random.fold_in(key, 105), (devices_all,), 0, spare)
    extra = jnp.minimum(jnp.minimum(extra_one, extra_two), extra_three)
    live = jnp.where(flat % 5 == 0, TILE_SLOTS, needed + extra)
    slot = jnp.arange(TILE_SLOTS, dtype=jnp.int32)
    halo_rank = jnp.clip(slot - RB, 0, None)[None, :]
    halo_cum = jnp.cumsum(halo_live.astype(jnp.int32), axis=1)
    halo_column = RB + jnp.sum((halo_cum[:, None, :] <= halo_rank[:, :, None]).astype(jnp.int32), axis=-1)
    count_live = jnp.sum(column_live.astype(jnp.int32), axis=1)
    pick = jax.random.randint(jax.random.fold_in(key, 107), (devices_all, TILE_SLOTS), 0, count_live[:, None])
    live_cum = jnp.cumsum(column_live.astype(jnp.int32), axis=1)
    random_column = jnp.sum((live_cum[:, None, :] <= pick[:, :, None]).astype(jnp.int32), axis=-1)
    random_row = jax.random.randint(jax.random.fold_in(key, 108), (devices_all, TILE_SLOTS), 0, RB)
    rows = jnp.where(slot < RB, slot, jnp.where(slot < live[:, None], random_row, -1))
    columns = jnp.where(slot < RB, slot, jnp.where(slot < needed[:, None], halo_column, jnp.where(slot < live[:, None], random_column, 0)))
    return (rows.reshape(-1).astype(jnp.int32), columns.reshape(-1).astype(jnp.int32), send_list.astype(jnp.int32))


def draw_tile_row(key, part):
    return layout(key)[0]


def draw_tile_col(key, part):
    return layout(key)[1]


def draw_send_list(key, part):
    return layout(key)[2]


def shard_levels(stream_key, shape, shards, smallest, largest):
    factor_of = 1.0
    for dim, shards_of in shards:
        draws = jax.random.uniform(jax.random.fold_in(jax.random.fold_in(stream_key, 6), dim), (shards_of,), jnp.float32, smallest / len(shards), largest / len(shards))
        factor_of = factor_of * jnp.repeat(jnp.exp(draws), shape[dim] // shards_of).reshape((-1,) + (1,) * (len(shape) - 1 - dim))
    return factor_of


def scatter_about(stream_key, shape, scale, bound, pieces=(), kind=jnp.bfloat16):
    drawn = scale * jax.random.normal(stream_key, shape, jnp.float32)
    if pieces:
        drawn = drawn * shard_levels(stream_key, shape, pieces, -0.22, 0.18)
    return jnp.clip(drawn, -bound, bound).astype(kind)


def setup_inputs(seed: int = 0) -> dict:
    key_of = jax.random.split(jax.random.key(seed), 9)
    return {
        "loads": scatter_about(key_of[0], (NRHS, DOFS), 1.0, 6.0, ((1, 32),), jnp.float32),
        "guess": scatter_about(key_of[1], (NRHS, DOFS), 0.5, 4.0, ((1, 32),), jnp.float32),
        "mass": jnp.clip(jnp.exp(math.log(4.0) - 2.0794415 * jax.random.uniform(key_of[2], (DOFS,), jnp.float32) ** shard_levels(key_of[2], (DOFS,), ((0, 32),), -0.2, 0.2)), 0.5, 4.0),
        "moduli": jnp.clip(jnp.exp(math.log(3.0) - 2.3025851 * jax.random.uniform(key_of[3], (DOFS,), jnp.float32) ** shard_levels(key_of[3], (DOFS,), ((0, 32),), -0.2, 0.2)), 0.3, 3.0),
        "tiles": scatter_about(key_of[4], (TILES, TB, TB), (TB * 3) ** -0.5, 0.21875, ((0, 32),), jnp.float32),
        "tile_row": draw_tile_row(jax.random.fold_in(key_of[8], 71), 0),
        "tile_col": draw_tile_col(jax.random.fold_in(key_of[8], 71), 0),
        "send_list": draw_send_list(jax.random.fold_in(key_of[8], 71), 0),
    }


def local_terms(operands):
    own, incoming, tiles_dev, rows_dev, cols_dev, moduli_dev = operands
    precise = lax.Precision.HIGHEST
    extent = RB + 4 * HALO
    extended = jnp.concatenate([own, jnp.transpose(incoming, (1, 0, 2))], 1)
    picked = jnp.take(extended, cols_dev, axis=1)
    row_onehot = (rows_dev[:, None] == jnp.arange(RB, dtype=jnp.int32)[None, :]).astype(jnp.float32)
    col_onehot = (cols_dev[:, None] == jnp.arange(extent, dtype=jnp.int32)[None, :]).astype(jnp.float32)
    strain_tiles = jnp.einsum("tij,ktj->kti", tiles_dev, picked, precision=precise)
    strain = jnp.einsum("tr,kti->kri", row_onehot, strain_tiles, precision=precise)
    stress = moduli_dev[None] * strain
    spread = jnp.einsum("tr,kri->kti", row_onehot, stress, precision=precise)
    pulled = jnp.einsum("tij,kti->ktj", tiles_dev, spread, precision=precise)
    return jnp.einsum("te,ktj->ekj", col_onehot, pulled, precision=precise)


def reference(loads, guess, mass, moduli, tiles, tile_row, tile_col, send_list):
    precise = lax.Precision.HIGHEST
    devices_all = N_GX * N_GY
    tiles_dev = tiles.reshape(devices_all, TILE_SLOTS, TB, TB)
    rows_dev = tile_row.reshape(devices_all, TILE_SLOTS)
    cols_dev = tile_col.reshape(devices_all, TILE_SLOTS)
    moduli_dev = moduli.reshape(devices_all, RB, TB)
    mass_dev = mass.reshape(devices_all, RB, TB)
    list_onehot = (send_list[:, :, :, None] == jnp.arange(RB, dtype=jnp.int32)).astype(jnp.float32)

    def shifted(grid, lower_src, upper_src, axis):
        if axis == 0:
            lower = jnp.concatenate([jnp.zeros_like(grid[:1, :, lower_src]), grid[:-1, :, lower_src]], 0)
            upper = jnp.concatenate([grid[1:, :, upper_src], jnp.zeros_like(grid[:1, :, upper_src])], 0)
        else:
            lower = jnp.concatenate([jnp.zeros_like(grid[:, :1, lower_src]), grid[:, :-1, lower_src]], 1)
            upper = jnp.concatenate([grid[:, 1:, upper_src], jnp.zeros_like(grid[:, :1, upper_src])], 1)
        return lower, upper

    def operate(vector):
        own = jnp.transpose(vector.reshape(NRHS, devices_all, RB, TB), (1, 0, 2, 3))
        packs = jnp.einsum("fdhr,fkri->fdhki", list_onehot, own, precision=precise)
        grid = packs.reshape(N_GX, N_GY, 4, HALO, NRHS, TB)
        first, second = shifted(grid, 1, 0, 0)
        third, fourth = shifted(grid, 3, 2, 1)
        incoming = jnp.stack([first, second, third, fourth], 2).reshape(devices_all, 4 * HALO, NRHS, TB)
        gathered = lax.map(local_terms, (own, incoming, tiles_dev, rows_dev, cols_dev, moduli_dev))
        returns = gathered[:, RB:].reshape(N_GX, N_GY, 4, HALO, NRHS, TB)
        first, second = shifted(returns, 1, 0, 0)
        third, fourth = shifted(returns, 3, 2, 1)
        returned = jnp.stack([first, second, third, fourth], 2).reshape(devices_all, 4, HALO, NRHS, TB)
        total = gathered[:, :RB] + jnp.einsum("fdhr,fdhki->frki", list_onehot, returned, precision=precise)
        result = mass_dev[:, None] * own + jnp.transpose(total, (0, 2, 1, 3))
        return jnp.transpose(result, (1, 0, 2, 3)).reshape(NRHS, devices_all * RB * TB)

    solution = guess
    residual = loads - operate(guess)
    direction = residual
    norm_now = jnp.sum(residual * residual, axis=1)
    for step in range(ITERS):
        image = operate(direction)
        alpha = norm_now / jnp.sum(direction * image, axis=1)
        solution = solution + alpha[:, None] * direction
        residual = residual - alpha[:, None] * image
        if step + 1 < ITERS:
            norm_next = jnp.sum(residual * residual, axis=1)
            direction = residual + (norm_next / norm_now)[:, None] * direction
            norm_now = norm_next
    return solution, residual
```

```python
import functools

import jax
import jax.numpy as jnp
from jax import lax
from jax.experimental import pallas as pl
from jax.experimental.pallas import tpu as pltpu
from jax.sharding import PartitionSpec as P

OPERATES = 3
PARTS = 2
CHUNKS = 8
MESH = pl.DeviceIdType.MESH
F32 = jnp.float32
BF16 = jnp.bfloat16


def split(value):
    high = value.astype(BF16)
    return high, (value - high.astype(F32)).astype(BF16)


def plan(tile_row, tile_col, send_list, blocks, depth):
    slots = tile_row.shape[0]
    extent = blocks + 4 * depth
    slot = jnp.arange(slots, dtype=jnp.int32)

    def ordered(key, other):
        before = (key[:, None] < key[None, :]) | (
            (key[:, None] == key[None, :]) & (slot[:, None] < slot[None, :])
        )
        rank = jnp.sum(before.astype(jnp.int32), axis=0)
        at = (rank[:, None] == slot[None, :]).astype(jnp.int32)
        pick = lambda v: jnp.sum(v[:, None] * at, axis=0)
        first = jnp.sum((key[:, None] < key[None, :]).astype(jnp.int32), axis=0)
        return pick(slot), pick(other), pick((rank > first).astype(jnp.int32))

    used = tile_row >= 0
    row_key = jnp.where(used, tile_row, blocks)
    col_key = jnp.where(used, tile_col, extent)
    row_slot, row_col, row_keep = ordered(row_key, tile_col)
    col_slot, col_row, col_keep = ordered(col_key, jnp.maximum(tile_row, 0))
    rows = jnp.arange(blocks, dtype=jnp.int32)
    cols = jnp.arange(extent, dtype=jnp.int32)
    row_last = jnp.sum((row_key[:, None] <= rows[None, :]).astype(jnp.int32), axis=0) - 1
    upto = jnp.sum((col_key[:, None] <= cols[None, :]).astype(jnp.int32), axis=0)
    here = jnp.sum((col_key[:, None] == cols[None, :]).astype(jnp.int32), axis=0)
    col_last = jnp.where(here > 0, upto - 1, slots)
    sends = send_list[0]
    send_index = jnp.maximum(sends, 0).reshape(-1)
    match = (sends[:, :, None] == rows[None, None, :]).astype(jnp.int32)
    where = jnp.sum(match * jnp.arange(depth, dtype=jnp.int32)[None, :, None], axis=1)
    back_index = jnp.where(jnp.sum(match, axis=1) > 0, where, depth).reshape(-1)
    table = jnp.concatenate(
        [row_slot, row_col, row_last, col_slot, col_row, col_last, send_index, back_index]
    )
    keep = jnp.concatenate([row_keep, col_keep]).astype(F32)
    return table, keep


def kernel(
    dims,
    table,
    keep,
    loads,
    guess,
    mass,
    moduli,
    tiles,
    out_solution,
    out_residual,
    staged,
    high,
    low,
    base,
    resid,
    first,
    second,
    extended,
    stress,
    scan,
    packs,
    incoming,
    returns,
    returned,
    sums_y,
    sums_x,
    tile_sem,
    pack_send,
    pack_recv,
    back_send,
    back_recv,
    y_send,
    y_recv,
    x_send,
    x_recv,
):
    blocks, block, slots, depth, cases, count_x, count_y = dims
    part = cases // PARTS
    extent = blocks + 4 * depth
    offsets = []
    at = 0
    for size in (slots, slots, blocks, slots, slots, extent, 4 * depth, 4 * blocks):
        offsets.append(at)
        at += size
    row_slot, row_col, row_last, col_slot, col_row, col_last, send_index, back_index = offsets
    my_x, my_y = lax.axis_index("gx"), lax.axis_index("gy")
    sides = (
        (my_x > 0, (my_x - 1, my_y)),
        (my_x < count_x - 1, (my_x + 1, my_y)),
        (my_y > 0, (my_x, my_y - 1)),
        (my_y < count_y - 1, (my_x, my_y + 1)),
    )

    step = slots // CHUNKS
    chunk_copies = [
        pltpu.make_async_copy(
            tiles.at[pl.ds(c * step, step)], staged.at[pl.ds(c * step, step)], tile_sem.at[c]
        )
        for c in range(CHUNKS)
    ]
    for copy in chunk_copies:
        copy.start()

    peers = [(lax.rem(my_x + k, count_x), my_y) for k in range(1, count_x)]
    peers += [(my_x, lax.rem(my_y + k, count_y)) for k in range(1, count_y)]
    barrier = pltpu.get_barrier_semaphore()
    for peer in peers:
        pl.semaphore_signal(barrier, inc=1, device_id=peer, device_id_type=MESH)

    for b in range(blocks):
        base[b] = guess[:, b * block : (b + 1) * block]
    for h in range(PARTS):
        scan[h, slots] = jnp.zeros((part, block), F32)
        for g in range(4):
            returned[h][g, depth] = jnp.zeros((part, block), F32)

    def rows_of(h):
        return pl.ds(h * part, part)

    def pack_copy(h, d):
        return pltpu.make_async_remote_copy(
            src_ref=packs.at[h, d],
            dst_ref=incoming.at[h, d ^ 1],
            send_sem=pack_send.at[h, d],
            recv_sem=pack_recv.at[h, d ^ 1],
            device_id=sides[d][1],
            device_id_type=MESH,
        )

    def back_copy(h, d):
        return pltpu.make_async_remote_copy(
            src_ref=returns.at[h, d],
            dst_ref=returned[h].at[d ^ 1, pl.ds(0, depth)],
            send_sem=back_send.at[h, d],
            recv_sem=back_recv.at[h, d ^ 1],
            device_id=sides[d][1],
            device_id_type=MESH,
        )

    def put_pack(vector, h):
        for d in range(4):
            for k in range(depth):
                packs[h, d, k] = vector[table[send_index + d * depth + k], rows_of(h), :]

    def start_pack(h):
        for d in range(4):

            @pl.when(sides[d][0])
            def _():
                pack_copy(h, d).start()

    def own_part(vector, h):
        for b in range(blocks):
            upper, lower = split(vector[b, rows_of(h), :])
            extended[h, b, :part] = upper
            extended[h, b, part:] = lower

    def product(left, slot, contract):
        dims_ = (((1,), (contract,)), ((), ()))
        both = lax.dot_general(left, high[slot], dims_, preferred_element_type=F32)
        rest = lax.dot_general(left[:part], low[slot], dims_, preferred_element_type=F32)
        return both[:part] + (both[part:] + rest)

    unroll = 8 if slots % 8 == 0 else 1

    def sweep(h, source, slot_at, index_at, keep_at, contract):
        def body(i, total):
            for u in range(unroll):
                p = i * unroll + u
                left = source[h, table[index_at + p]]
                total = product(left, table[slot_at + p], contract) + keep[keep_at + p] * total
                scan[h, p] = total
            return total

        lax.fori_loop(0, slots // unroll, body, jnp.zeros((part, block), F32))

    def compute(h):
        for g in range(4):

            @pl.when(sides[g][0])
            def _():
                pack_copy(h, g ^ 1).wait_recv()

        for g in range(4):
            for k in range(depth):
                upper, lower = split(incoming[h, g, k])
                extended[h, blocks + g * depth + k, :part] = upper
                extended[h, blocks + g * depth + k, part:] = lower
        sweep(h, extended, row_slot, row_col, 0, 1)
        for b in range(blocks):
            value = scan[h, table[row_last + b]] * moduli[:, b * block : (b + 1) * block]
            upper, lower = split(value)
            stress[h, b, :part] = upper
            stress[h, b, part:] = lower
        sweep(h, stress, col_slot, col_row, slots, 0)
        for g in range(4):
            for k in range(depth):
                returns[h, g, k] = scan[h, table[col_last + blocks + g * depth + k]]

            @pl.when(sides[g][0])
            def _():
                back_copy(h, g).start()

    def finish(h):
        for g in range(4):

            @pl.when(sides[g][0])
            def _():
                back_copy(h, g ^ 1).wait_recv()
                pack_copy(h, g).wait_send()
                back_copy(h, g).wait_send()

    def image_of(vector, h, b):
        total = scan[h, table[col_last + b]]
        for g in range(4):
            total += returned[h][g, table[back_index + g * blocks + b]]
        return total + mass[:, b * block : (b + 1) * block] * vector[b, rows_of(h), :]

    def fold(value):
        total = value[:, :128]
        for c in range(1, block // 128):
            total += value[:, c * 128 : (c + 1) * 128]
        return total

    def sum_copies(buffer, send, recv, n, axis, me, count):
        def copy(k, sending):
            other = lax.rem(me + (k if sending else count - k), count)
            target = (other, my_y) if axis == 0 else (my_x, other)
            return pltpu.make_async_remote_copy(
                src_ref=buffer.at[n, me],
                dst_ref=buffer.at[n, me if sending else other],
                send_sem=send.at[n, k],
                recv_sem=recv.at[n, k],
                device_id=target,
                device_id_type=MESH,
            )

        return copy

    def start_sum(n, axis, value):
        buffer, send, recv, me, count = (
            (sums_x, x_send, x_recv, my_x, count_x)
            if axis == 0
            else (sums_y, y_send, y_recv, my_y, count_y)
        )
        buffer[n, me] = value
        copy = sum_copies(buffer, send, recv, n, axis, me, count)
        for k in range(1, count):
            copy(k, True).start()

    def end_sum(n, axis):
        buffer, send, recv, me, count = (
            (sums_x, x_send, x_recv, my_x, count_x)
            if axis == 0
            else (sums_y, y_send, y_recv, my_y, count_y)
        )
        copy = sum_copies(buffer, send, recv, n, axis, me, count)
        for k in range(1, count):
            copy(k, False).wait_recv()
            copy(k, True).wait_send()
        return jnp.sum(buffer[n], axis=0)

    def packed(norms, products):
        both = jnp.concatenate(norms + products, axis=0)
        return jnp.broadcast_to(jnp.sum(both.T, axis=0, keepdims=True), (8, 128))

    def columns(value):
        spread = jnp.broadcast_to(value[:1], (128, 128)).T
        return spread[:cases], spread[cases : 2 * cases]

    for h in range(PARTS):
        put_pack(base, h)
    pl.semaphore_wait(barrier, len(peers))
    for h in range(PARTS):
        start_pack(h)
    for h in range(PARTS):
        own_part(base, h)

    for c in range(CHUNKS):
        chunk_copies[c].wait()

        def convert(i, carry, c=c):
            upper, lower = split(staged[c * step + i])
            high[c * step + i] = upper
            low[c * step + i] = lower
            return carry

        lax.fori_loop(0, step, convert, 0)

    for h in range(PARTS):
        compute(h)
    for h in range(PARTS):
        finish(h)
        for b in range(blocks):
            resid[b, rows_of(h), :] = loads[
                rows_of(h), b * block : (b + 1) * block
            ] - image_of(base, h, b)
        put_pack(resid, h)
        start_pack(h)
        own_part(resid, h)

    for h in range(PARTS):
        compute(h)
    norms, products = [], []
    for h in range(PARTS):
        finish(h)
        norm = jnp.zeros((part, 128), F32)
        inner = jnp.zeros((part, 128), F32)
        for b in range(blocks):
            value = image_of(resid, h, b)
            first[b, rows_of(h), :] = value
            r = resid[b, rows_of(h), :]
            norm += fold(r * r)
            inner += fold(r * value)
        put_pack(first, h)
        start_pack(h)
        own_part(first, h)
        norms.append(norm)
        products.append(inner)
    start_sum(0, 1, packed(norms, products))

    compute(0)
    start_sum(0, 0, end_sum(0, 1))
    for h in range(1, PARTS):
        compute(h)
    norm_now, product_now = columns(end_sum(0, 0))
    alpha = norm_now / product_now
    alpha_wide = jnp.concatenate([alpha] * (block // 128), axis=1)
    norms, products = [], []
    for h in range(PARTS):
        finish(h)
        scale = alpha_wide[h * part : (h + 1) * part]
        norm = jnp.zeros((part, 128), F32)
        inner = jnp.zeros((part, 128), F32)
        for b in range(blocks):
            w = first[b, rows_of(h), :]
            r = resid[b, rows_of(h), :] - scale * w
            image = w - scale * image_of(first, h, b)
            second[b, rows_of(h), :] = image
            norm += fold(r * r)
            inner += fold(r * image)
        norms.append(norm)
        products.append(inner)
    start_sum(1, 1, packed(norms, products))
    start_sum(1, 0, end_sum(1, 1))
    norm_next, product_next = columns(end_sum(1, 0))
    ratio = norm_next / norm_now
    alpha_next = norm_next / (product_next - ratio * norm_next / alpha)
    ratio_wide = jnp.concatenate([ratio] * (block // 128), axis=1)
    next_wide = jnp.concatenate([alpha_next] * (block // 128), axis=1)
    for b in range(blocks):
        cols = slice(b * block, (b + 1) * block)
        r0 = resid[b]
        w = first[b]
        r1 = r0 - alpha_wide * w
        out_solution[:, cols] = (base[b] + alpha_wide * r0) + next_wide * (r1 + ratio_wide * r0)
        out_residual[:, cols] = r1 - next_wide * (second[b] + ratio_wide * w)


def on_device(loads, guess, mass, moduli, tiles, tile_row, tile_col, send_list):
    cases = loads.shape[0]
    slots, block = tiles.shape[0], tiles.shape[1]
    blocks = mass.shape[0] // block
    depth = send_list.shape[2]
    extent = blocks + 4 * depth
    count_x, count_y = lax.axis_size("gx"), lax.axis_size("gy")
    part = cases // PARTS
    table, keep = plan(tile_row, tile_col, send_list, blocks, depth)
    dims = (blocks, block, slots, depth, cases, count_x, count_y)
    vmem = pl.BlockSpec(memory_space=pltpu.VMEM)
    smem = pl.BlockSpec(memory_space=pltpu.SMEM)
    return pl.pallas_call(
        functools.partial(kernel, dims),
        out_shape=(
            jax.ShapeDtypeStruct(loads.shape, F32),
            jax.ShapeDtypeStruct(loads.shape, F32),
        ),
        in_specs=[smem, smem, vmem, vmem, vmem, vmem, pl.BlockSpec(memory_space=pl.ANY)],
        out_specs=(vmem, vmem),
        scratch_shapes=[
            pltpu.VMEM((slots, block, block), F32),
            pltpu.VMEM((slots, block, block), BF16),
            pltpu.VMEM((slots, block, block), BF16),
            pltpu.VMEM((blocks, cases, block), F32),
            pltpu.VMEM((blocks, cases, block), F32),
            pltpu.VMEM((blocks, cases, block), F32),
            pltpu.VMEM((blocks, cases, block), F32),
            pltpu.VMEM((PARTS, extent, 2 * part, block), BF16),
            pltpu.VMEM((PARTS, blocks, 2 * part, block), BF16),
            pltpu.VMEM((PARTS, slots + 1, part, block), F32),
            pltpu.VMEM((PARTS, 4, depth, part, block), F32),
            pltpu.VMEM((PARTS, 4, depth, part, block), F32),
            pltpu.VMEM((PARTS, 4, depth, part, block), F32),
            tuple(pltpu.VMEM((4, depth + 1, part, block), F32) for _ in range(PARTS)),
            pltpu.VMEM((2, count_y, 8, 128), F32),
            pltpu.VMEM((2, count_x, 8, 128), F32),
            pltpu.SemaphoreType.DMA((CHUNKS,)),
            pltpu.SemaphoreType.DMA((PARTS, 4)),
            pltpu.SemaphoreType.DMA((PARTS, 4)),
            pltpu.SemaphoreType.DMA((PARTS, 4)),
            pltpu.SemaphoreType.DMA((PARTS, 4)),
            pltpu.SemaphoreType.DMA((2, count_y)),
            pltpu.SemaphoreType.DMA((2, count_y)),
            pltpu.SemaphoreType.DMA((2, count_x)),
            pltpu.SemaphoreType.DMA((2, count_x)),
        ],
        compiler_params=pltpu.CompilerParams(
            collective_id=0, has_side_effects=True, vmem_limit_bytes=56 * 1024 * 1024
        ),
    )(
        table,
        keep,
        loads,
        guess,
        mass.reshape(1, -1),
        moduli.reshape(1, -1),
        tiles,
    )


def solution(mesh):
    return jax.shard_map(
        on_device,
        mesh=mesh,
        in_specs=(
            P(None, ("gx", "gy")),
            P(None, ("gx", "gy")),
            P(("gx", "gy")),
            P(("gx", "gy")),
            P(("gx", "gy"), None, None),
            P(("gx", "gy")),
            P(("gx", "gy")),
            P(("gx", "gy"), None, None),
        ),
        out_specs=(P(None, ("gx", "gy")), P(None, ("gx", "gy"))),
        check_vma=False,
    )
```
